768 devices in a mesh: grp: 48 (over z, y_lo, core), shard: 16 (over y_hi, x).
Axes of the slice: x: 4, y: 8 (y_hi: 4, y_lo: 2; y = y_hi * 2 + y_lo), z: 12, core: 2. Of those that a mesh axis runs over, the one named last changes fastest.
Arguments:
- gradient: bfloat16 [48, 16, 384, 1024], P('grp', None, 'shard'), may hold values from -300 to 300
- momentum: float32 [48, 16, 384, 1024], P('grp', None, 'shard'), may hold values from -6 to 6
- owner: int32 [48, 16, 1], P('grp'), may hold values from 0 to 15; in each aligned block of 16 rows (0 to 15, 16 to 31, ..., all dimensions but the last counted through in order) at most 2 rows name the same one
Outputs:
- update: bfloat16 [48, 16, 384, 1024], P('grp', None, 'shard')
- momentum_out: float32 [48, 16, 384, 1024], P('grp', None, 'shard')
- slot_rms: float32 [48, 16, 2], P('grp', 'shard')
The draws below stay inside these ranges and needn't reach their ends.
Inputs may be any that keep to these rules, and one draw needn't show every extreme that they name: `owner`: in every group no index of shard owns more than 2 matrices, and in some group some index owns exactly 2.
All inputs are finite; a program needn't handle non-finite values.
Results may differ from the reference program's by a relative error of at most 0.0085.
Values may be sent and summed in bfloat16 or wider, within the bound.
A program may use at most 32 MiB of HBM per device.

```python
import math
import jax
import jax.numpy as jnp
import numpy as np
from jax import lax

ROWS = 384
COLS = 1024
ITERS = 3
MATS = 16
CAP = 2
GROUPS = 48
N_SHARD = 16


def draw_gradient(key, part):
    normal_base = jnp.clip(jax.random.normal(jax.random.fold_in(key, 11), (GROUPS, MATS, ROWS, COLS), jnp.float32), -5.0, 5.0)
    position = (jnp.arange(GROUPS)[:, None] * ROWS + jnp.arange(ROWS)[None, :]).astype(jnp.float32) / (GROUPS * ROWS)
    rising = (1.0 + 2.0 * position)[:, None, :, None]
    matrix_scale = jnp.exp(jax.random.uniform(jax.random.fold_in(key, 12), (GROUPS, MATS, 1, 1), jnp.float32, math.log(0.5), math.log(2.0)))
    block_level = jnp.exp(jax.random.uniform(jax.random.fold_in(key, 15), (N_SHARD,), jnp.float32, math.log(0.2), math.log(5.0)))
    block_scale = jnp.repeat(block_level, ROWS // N_SHARD)[None, None, :, None]
    values = normal_base * rising * matrix_scale * block_scale
    return values.astype(jnp.bfloat16)


def block_levels(own_key, shape, cuts, smallest, largest):
    gain, own = 1.0, jax.random.fold_in(own_key, 6)
    for axis_at, parts in cuts:
        draws = jnp.exp(jax.random.uniform(jax.random.fold_in(own, axis_at), (parts,), jnp.float32, smallest / len(cuts), largest / len(cuts)))
        gain = gain * jnp.repeat(draws, shape[axis_at] // parts).reshape([-1 if axis == axis_at else 1 for axis in range(len(shape))])
    return gain


def shared_out(key, own, number, rows, count, top, limit, skew):
    sequence = jax.random.permutation(key, count)
    crowded, common = portions_of(count, rows * top, limit, skew, True), portions_of(count, rows * top, limit, skew, False)
    places = jnp.arange(count)

    def named(sizes, rotation):
        used = int((sizes > 0).sum())
        fixed = max(1, used // 4)
        moved = fixed + (places - fixed + rotation * (used - fixed)) % max(1, count - fixed)
        return jnp.zeros((count,), jnp.int32).at[sequence[jnp.where(places < fixed, places, moved)]].set(jnp.asarray(sizes, jnp.int32))

    sizes = jnp.where(number % 4 == 0, named(crowded, number // 4), named(common, number - number // 4 - 1))
    mixed = jax.random.permutation(jax.random.fold_in(own, 3), count)
    source_of, receiver = mixed[0:count // 2 * 2:2], mixed[1:count // 2 * 2:2]
    room = jnp.minimum(sizes[source_of] - 1, limit - sizes[receiver]) // 2
    room = jnp.where((source_of == sequence[0]) | (receiver == sequence[0]) | (sizes[receiver] == 0), 0, jnp.maximum(room, 0))
    moved = jax.random.randint(jax.random.fold_in(own, 4), (count // 2,), 0, 1 << 20) % (room + 1)
    sizes = sizes.at[source_of].add(-moved).at[receiver].add(moved)
    labels = jnp.searchsorted(jnp.cumsum(sizes), jnp.arange(rows * top), side="right").astype(jnp.int32)
    table = labels.reshape(top, rows).T
    table = table[jax.random.permutation(jax.random.fold_in(own, 1), rows)]
    rotation = jax.random.randint(jax.random.fold_in(own, 2), (rows, 1), 0, top)
    return jnp.take_along_axis(table, (jnp.arange(top)[None, :] + rotation) % top, axis=1)


def portions_of(number_of, total, reach, slope, full):
    portions = [(1 << 20) // math.isqrt(grade ** slope) + 1 for grade in range(1, number_of + 1)]
    largest = reach if full else min(reach, max(-(-total // number_of), total * portions[0] // sum(portions)))
    least = 1 if total - largest >= number_of - 1 else 0
    given, rest = [largest] + [least] * (number_of - 1), total - largest - least * (number_of - 1)
    while rest > 0:
        candidates = [i for i in range(1, number_of) if given[i] < largest] or [i for i in range(1, number_of) if given[i] < reach]
        mass, remaining = sum([portions[i] for i in candidates]), rest
        for i in candidates:
            addition = min(reach - given[i], max(1, remaining * portions[i] // mass), rest)
            given[i] = given[i] + addition
            rest = rest - addition
    return np.array(given)


def centred(own_key, dims, scale, most, split=(), kind=jnp.bfloat16):
    gain = block_levels(own_key, dims, split, -0.22, 0.18) if split else 1.0
    result = jax.random.normal(own_key, dims, jnp.float32) * scale * gain
    return jnp.minimum(jnp.maximum(result, -most), most).astype(kind)


def setup_inputs(seed: int = 0) -> dict:
    key_list = jax.random.split(jax.random.key(seed), 4)
    gradient = draw_gradient(jax.random.fold_in(key_list[3], 71), 0)
    momentum = centred(key_list[1], (GROUPS, MATS, ROWS, COLS), 1.0, 6.0, ((0, 48), (2, 16)), jnp.float32)
    owner_keys = jax.random.split(jax.random.fold_in(key_list[2], 1), GROUPS * MATS // MATS)
    owner_turns = jax.random.permutation(jax.random.fold_in(key_list[2], 3), GROUPS * MATS // MATS)
    owner = jax.vmap(lambda own, number: shared_out(jax.random.fold_in(key_list[2], 2), own, number, MATS, N_SHARD, 1, CAP, 2))(owner_keys, owner_turns).reshape((GROUPS, MATS, 1))
    return dict(gradient=gradient, momentum=momentum, owner=owner)


QUINTIC_A = 3.4445
QUINTIC_B = -4.775
QUINTIC_C = 2.0315
MOMENTUM_DECAY = 0.95
CLIP_LEVEL = 0.5

def newton(matrix):
    wide = matrix.astype(jnp.float32)
    square_sum = jnp.sum(wide * wide)
    iterate = (wide / (jnp.sqrt(square_sum) + 1e-07)).astype(jnp.bfloat16)
    for repeat in range(ITERS):
        gram_matrix = jnp.dot(iterate, iterate.T, preferred_element_type=jnp.float32).astype(jnp.bfloat16)
        squared = jnp.dot(gram_matrix, gram_matrix, preferred_element_type=jnp.float32)
        blended = (QUINTIC_B * gram_matrix.astype(jnp.float32) + QUINTIC_C * squared).astype(jnp.bfloat16)
        iterate = (QUINTIC_A * iterate.astype(jnp.float32) + jnp.dot(blended, iterate, preferred_element_type=jnp.float32)).astype(jnp.bfloat16)
    return (iterate, square_sum)

def reference(gradient, momentum, owner):
    grad_wide = gradient.astype(jnp.float32)
    mean_square = jnp.sum(grad_wide * grad_wide) / (GROUPS * MATS * ROWS * COLS)
    clip_factor = jnp.minimum(jnp.float32(1.0), CLIP_LEVEL / jnp.sqrt(mean_square + 1e-06))
    momentum_out = MOMENTUM_DECAY * momentum + clip_factor * grad_wide
    nesterov = (clip_factor * grad_wide + MOMENTUM_DECAY * momentum_out).astype(jnp.bfloat16)
    stacked = nesterov.reshape(GROUPS * MATS, ROWS, COLS)
    ortho, squares = lax.map(newton, stacked)
    update = (ortho.astype(jnp.float32) * math.sqrt(COLS)).astype(jnp.bfloat16).reshape(GROUPS, MATS, ROWS, COLS)
    owners = owner[:, :, 0]
    owner_hot = (owners[:, :, None] == jnp.arange(N_SHARD, dtype=jnp.int32)[None, None, :]).astype(jnp.int32)
    ranking = lax.optimization_barrier(jnp.sum((jnp.cumsum(owner_hot, axis=1) - owner_hot) * owner_hot, axis=2))
    slot_hot = (ranking[:, :, None] == jnp.arange(CAP, dtype=jnp.int32)[None, None, :]).astype(jnp.float32)
    matrix_rms = jnp.sqrt(squares.reshape(GROUPS, MATS)) / math.sqrt(ROWS * COLS)
    slot_rms = lax.optimization_barrier(jnp.sum(owner_hot.astype(jnp.float32)[:, :, :, None] * slot_hot[:, :, None, :] * matrix_rms[:, :, None, None], axis=1))
    return (update, momentum_out, slot_rms)
```

```python
import functools
import math

import jax
import jax.numpy as jnp
from jax import lax
from jax.experimental import pallas as pl
from jax.experimental.pallas import tpu as pltpu
from jax.sharding import Mesh
from jax.sharding import PartitionSpec as P

ITERS = 3
CAP = 2
QUINTIC_A = 3.4445
QUINTIC_B = -4.775
QUINTIC_C = 2.0315
MOMENTUM_DECAY = 0.95
CLIP_LEVEL = 0.5

AXES = ("z", "yl", "c", "yh", "x")
SHARD = ("yh", "x")
GRP = ("z", "yl", "c")
LANES = 128


def displacements(yh_size, x_size):
    his = sorted(range(yh_size), key=lambda h: -min(2 * h + 1, 2 * (yh_size - h) - 1))
    return [(h, dx) for dx in range(x_size) for h in his]


def kernel(sizes, count, g_hbm, m_hbm, owner_ref, upd_ref, mom_ref, slot_ref,
           g_v, m_v, nest, got, mat, back, gram_v, part, p1, p2, p3, squares, square_row,
           load_sem, send_sem, recv_sem, back_send, back_recv, small_send, small_recv):
    z_size, yh_size, x_size = sizes
    mats, rows, cols = g_v.shape
    shards = yh_size * x_size
    z, yl, c = lax.axis_index("z"), lax.axis_index("yl"), lax.axis_index("c")
    yh, x = lax.axis_index("yh"), lax.axis_index("x")
    me = yh * x_size + x
    order = displacements(yh_size, x_size)

    def peer(k):
        h, dx = order[k]
        there_h = lax.rem(yh + h * (1 - yl) + (yh_size - h) * yl, yh_size)
        there_x = lax.rem(x + dx * (1 - yl) + (x_size - dx) * yl, x_size)
        return there_h, there_x

    def where(k):
        there_h, there_x = peer(k)
        return {"z": z, "yl": 1 - yl, "c": c, "yh": there_h, "x": there_x}

    def index(k):
        there_h, there_x = peer(k)
        return there_h * x_size + there_x

    quad = [{"z": z, "yl": lax.rem(yl + a, 2), "c": lax.rem(c + b, 2), "yh": yh, "x": x} for a, b in ((0, 1), (1, 0), (1, 1))]
    column = [{"z": lax.rem(z + k, z_size), "yl": yl, "c": c, "yh": yh, "x": x} for k in range(1, z_size)]

    half = mats // 2
    loads = []
    for part_at in range(2):
        span = pl.ds(part_at * half, half)
        loads.append(pltpu.make_async_copy(g_hbm.at[span], g_v.at[span], load_sem.at[part_at]))
    loads.append(pltpu.make_async_copy(m_hbm, m_v, load_sem.at[2]))
    for load in loads:
        load.start()

    barrier = pltpu.get_barrier_semaphore()
    for device in [quad[0], quad[2], *column]:
        pl.semaphore_signal(barrier, inc=1, device_id=device)
    for k in range(shards):
        pl.semaphore_signal(barrier, inc=1, device_id=where(k))

    def squared(first):
        def add(j, total):
            wide = g_v[first + j].astype(jnp.float32)
            return total + wide * wide
        return add

    total = jnp.zeros((rows, cols), jnp.float32)
    for part_at in range(2):
        loads[part_at].wait()
        total = lax.fori_loop(0, half, squared(part_at * half), total)
    part[0] = jnp.full((1, LANES), jnp.sum(total), jnp.float32)

    pl.semaphore_wait(barrier, 2 + len(column) + shards)

    def remote(source, target, sender, receiver, device):
        return pltpu.make_async_remote_copy(source, target, sender, receiver, device_id=device)

    for k, device in enumerate(quad):
        remote(part.at[0], p1.at[k], small_send.at[0], small_recv.at[0], device).start()
    remote(p1, p1, small_send.at[0], small_recv.at[0], quad[0]).wait()
    part[1] = part[0] + jnp.sum(p1[...], axis=0)
    for k, device in enumerate(column):
        remote(part.at[1], p2.at[k], small_send.at[1], small_recv.at[1], device).start()
    remote(p2, p2, small_send.at[1], small_recv.at[1], column[0]).wait()
    part[2] = part[1] + jnp.sum(p2[...], axis=0)
    for k in range(shards):
        remote(part.at[2], p3.at[k], small_send.at[2], small_recv.at[2], where(k)).start()
    loads[2].wait()
    remote(p3, p3, small_send.at[2], small_recv.at[2], where(0)).wait()

    mean = jnp.sum(p3[...], axis=0) / count
    clip = jnp.max(jnp.minimum(1.0, CLIP_LEVEL / jnp.sqrt(mean + 1e-06)))

    for k in range(shards):
        j = index(k)
        pulled = clip * g_v[j].astype(jnp.float32)
        kept = MOMENTUM_DECAY * m_v[j] + pulled
        m_v[j] = kept
        nest[k] = (pulled + MOMENTUM_DECAY * kept).astype(jnp.bfloat16)
        remote(nest.at[k], got.at[k], send_sem, recv_sem.at[k], where(k)).start()
    mom_copy = pltpu.make_async_copy(m_v, mom_ref, load_sem.at[3])
    mom_copy.start()

    total = jnp.zeros((rows, cols), jnp.float32)
    for k in range(shards):
        remote(nest.at[k], got.at[k], send_sem, recv_sem.at[k], where(k)).wait_recv()
        wide = got[k].astype(jnp.float32)
        total = total + wide * wide
    square_sum = jnp.sum(total)
    norm = jnp.sqrt(jnp.full((1, LANES), square_sum, jnp.float32))
    scale = jnp.max(1.0 / (norm + 1e-07))
    square_row[...] = norm
    for k in range(shards):
        remote(square_row, squares.at[k], small_send.at[3], small_recv.at[3], where(k)).start()
    for k in range(0, shards, 2):
        pair = jnp.concatenate([got[k].astype(jnp.float32), got[k + 1].astype(jnp.float32)], axis=0)
        mat[pl.ds(k * rows, 2 * rows), :] = (pair * scale).astype(jnp.bfloat16)

    over = (((1,), (1,)), ((), ()))
    plain = (((1,), (0,)), ((), ()))
    full = shards * rows
    for repeat in range(ITERS):
        iterate = mat[...]
        gram_v[...] = lax.dot_general(iterate, iterate, over, preferred_element_type=jnp.float32).astype(jnp.bfloat16)
        gram = gram_v[...]
        squared_gram = lax.dot_general(gram, gram, plain, preferred_element_type=jnp.float32)
        gram_v[...] = (QUINTIC_B * gram.astype(jnp.float32) + QUINTIC_C * squared_gram).astype(jnp.bfloat16)
        if repeat < ITERS - 1:
            product = lax.dot_general(gram_v[...], iterate, plain, preferred_element_type=jnp.float32)
            mat[...] = (QUINTIC_A * iterate.astype(jnp.float32) + product).astype(jnp.bfloat16)

    chunk = 4 if shards % 4 == 0 else 2
    for first in range(0, shards, chunk):
        span = pl.ds(first * rows, chunk * rows)
        product = lax.dot_general(gram_v[span, :], mat[...], plain, preferred_element_type=jnp.float32)
        final = (QUINTIC_A * mat[span, :].astype(jnp.float32) + product) * math.sqrt(cols)
        for k in range(first, first + chunk):
            back[k] = final[(k - first) * rows:(k - first + 1) * rows].astype(jnp.bfloat16)
            remote(back.at[k], upd_ref.at[me], back_send, back_recv, where(k)).start()

    remote(squares, squares, small_send.at[3], small_recv.at[3], where(0)).wait()
    taken = jnp.int32(0)
    slots = [jnp.zeros((1, LANES), jnp.float32) for _ in range(CAP)]
    rms = [squares[k] / math.sqrt(full * cols) for k in range(shards)]
    named = [(index(k), rms[k]) for k in range(shards)]
    for j in range(mats):
        mine = (owner_ref[0, j] == me).astype(jnp.int32)
        rank = taken
        taken = taken + mine
        for s in range(CAP):
            hit = mine * (rank == s).astype(jnp.int32)
            for place, value in named:
                slots[s] = slots[s] + (hit * (place == j).astype(jnp.int32)).astype(jnp.float32) * value
    lane = lax.broadcasted_iota(jnp.int32, (1, LANES), 1)
    slot_ref[...] = jnp.where(lane == 0, slots[0], slots[1])

    remote(nest, got, send_sem, recv_sem.at[0], where(0)).wait_send()
    mom_copy.wait()
    remote(upd_ref, upd_ref, back_send, back_recv, where(0)).wait()


def body(gradient, momentum, owner):
    sizes = (lax.axis_size("z"), lax.axis_size("yh"), lax.axis_size("x"))
    shards = sizes[1] * sizes[2]
    _, mats, rows, cols = gradient.shape
    count = mats * rows * cols * shards * lax.axis_size(GRP)
    full = rows * shards
    anywhere, vmem = pl.BlockSpec(memory_space=pl.ANY), pl.BlockSpec(memory_space=pltpu.VMEM)
    dma = pltpu.SemaphoreType.DMA
    update, momentum_out, slots = pl.pallas_call(
        functools.partial(kernel, sizes, count),
        name="muon",
        out_shape=(
            jax.ShapeDtypeStruct((mats, rows, cols), jnp.bfloat16),
            jax.ShapeDtypeStruct((mats, rows, cols), jnp.float32),
            jax.ShapeDtypeStruct((1, LANES), jnp.float32),
        ),
        in_specs=[anywhere, anywhere, pl.BlockSpec(memory_space=pltpu.SMEM)],
        out_specs=(vmem, anywhere, vmem),
        scratch_shapes=[
            pltpu.VMEM((mats, rows, cols), jnp.bfloat16),
            pltpu.VMEM((mats, rows, cols), jnp.float32),
            pltpu.VMEM((shards, rows, cols), jnp.bfloat16),
            pltpu.VMEM((shards, rows, cols), jnp.bfloat16),
            pltpu.VMEM((full, cols), jnp.bfloat16),
            pltpu.VMEM((shards, rows, cols), jnp.bfloat16),
            pltpu.VMEM((full, full), jnp.bfloat16),
            pltpu.VMEM((3, 1, LANES), jnp.float32),
            pltpu.VMEM((3, 1, LANES), jnp.float32),
            pltpu.VMEM((sizes[0] - 1, 1, LANES), jnp.float32),
            pltpu.VMEM((shards, 1, LANES), jnp.float32),
            pltpu.VMEM((shards, 1, LANES), jnp.float32),
            pltpu.VMEM((1, LANES), jnp.float32),
            dma((4,)),
            dma,
            dma((shards,)),
            dma,
            dma,
            dma((4,)),
            dma((4,)),
        ],
        compiler_params=pltpu.CompilerParams(collective_id=0, has_side_effects=True),
    )(gradient[0], momentum[0], owner.reshape(1, mats))
    return update[None], momentum_out[None], slots[:, None, :CAP]


def solution(mesh):
    finer = Mesh(mesh.devices.reshape(12, 2, 2, 4, 4), AXES)
    return jax.shard_map(
        body,
        mesh=finer,
        in_specs=(P(GRP, None, SHARD, None), P(GRP, None, SHARD, None), P(GRP, None, None)),
        out_specs=(P(GRP, None, SHARD, None), P(GRP, None, SHARD, None), P(GRP, SHARD, None)),
        check_vma=False,
    )
```

```python
import functools
import math

import jax
import jax.numpy as jnp
from jax import lax
from jax.experimental import pallas as pl
from jax.experimental.pallas import tpu as pltpu
from jax.sharding import Mesh
from jax.sharding import PartitionSpec as P

ITERS = 3
CAP = 2
QUINTIC_A = 3.4445
QUINTIC_B = -4.775
QUINTIC_C = 2.0315
MOMENTUM_DECAY = 0.95
CLIP_LEVEL = 0.5

AXES = ("z", "yl", "c", "yh", "x")
SHARD = ("yh", "x")
GRP = ("z", "yl", "c")
LANES = 128


def early_blocks(z, c, shards):
    return (1 - c) * (shards - shards // 4 * (1 - lax.div(16 - z, 12)))


def kernel(sizes, count, g_hbm, m_hbm, owner_hbm, upd_ref, mom_ref, slot_ref,
           owner_ref, pair_v, m_v, got_pair, nest, got, mat, back, gram_v, part, p1, p2, p3, whole, squares, square_row,
           g_sem, load_sem, send_sem, pair_recv, recv_sem, back_send, back_recv, small_send, small_recv):
    z_size, yh_size, x_size = sizes
    mats, rows, cols = m_v.shape
    shards = yh_size * x_size
    z, yl, c = lax.axis_index("z"), lax.axis_index("yl"), lax.axis_index("c")
    yh, x = lax.axis_index("yh"), lax.axis_index("x")
    me = yh * x_size + x
    early = early_blocks(z, c, shards)
    turn = me + 2 * yl

    def peer(k):
        h, dx = lax.rem(k + 1, yh_size), lax.div(k, yh_size)
        there_h = lax.rem(yh + h * (1 - yl) + (yh_size - h) * yl, yh_size)
        there_x = lax.rem(x + dx * (1 - yl) + (x_size - dx) * yl, x_size)
        return there_h, there_x

    def where(k):
        there_h, there_x = peer(jnp.int32(k))
        return {"z": z, "yl": 1 - yl, "c": c, "yh": there_h, "x": there_x}

    def index(k):
        there_h, there_x = peer(jnp.int32(k))
        return there_h * x_size + there_x

    def remote(source, target, sender, receiver, device):
        return pltpu.make_async_remote_copy(source, target, sender, receiver, device_id=device)

    here = {"z": z, "yl": yl, "c": c, "yh": yh, "x": x}
    other_core = {**here, "c": 1 - c}
    far_first = sorted(range(1, z_size), key=lambda k: -min(k, z_size - k))
    column = {k: {**here, "z": lax.rem(z + k, z_size)} for k in far_first}
    same_lo = {k: {**here, "yh": lax.rem(yh + k // x_size, yh_size), "x": lax.rem(x + k % x_size, x_size)} for k in range(1, shards)}

    barrier = pltpu.get_barrier_semaphore()

    @pl.when(c == 1)
    def _():
        for device in (*column.values(), *same_lo.values()):
            pl.semaphore_signal(barrier, inc=1, device_id=device)

    for k in range(shards):
        pl.semaphore_signal(barrier, inc=1, device_id=where(k))
    pl.semaphore_signal(barrier, inc=1, device_id=other_core)

    def g_load(k):
        return pltpu.make_async_copy(g_hbm.at[index(k)], pair_v.at[k, 0], g_sem.at[k])

    for k in range(shards):
        g_load(k).start()
    m_load = pltpu.make_async_copy(m_hbm, m_v, load_sem.at[0])
    m_load.start()
    owner_load = pltpu.make_async_copy(owner_hbm, owner_ref, load_sem.at[1])
    owner_load.start()

    def add_gradient(k, total):
        g_load(k).wait()
        wide = pair_v[k, 0].astype(jnp.float32)
        return total + wide * wide

    nothing = jnp.zeros((rows, cols), jnp.float32)
    part[0] = jnp.full((1, LANES), jnp.sum(lax.fori_loop(0, shards, add_gradient, nothing)), jnp.float32)

    pl.semaphore_wait(barrier, 1 + shards + c * (len(column) + len(same_lo)))

    def part_copy():
        return remote(part.at[0], p1.at[0], small_send.at[0], small_recv.at[0], other_core)

    def sum_copy():
        return remote(whole.at[0], whole.at[0], small_send.at[4], small_recv.at[4], other_core)

    @pl.when(c == 0)
    def _():
        part_copy().start()

    m_load.wait()

    def send_pair(i, _):
        k = lax.rem(i + turn, early)
        pair_v[k, 1] = m_v[index(k)].astype(jnp.bfloat16)
        remote(pair_v.at[k], got_pair.at[k], send_sem.at[k], pair_recv.at[k], where(k)).start()
        return 0

    lax.fori_loop(0, early, send_pair, 0)

    @pl.when(c == 0)
    def _():
        part_copy().wait_send()
        sum_copy().wait_recv()

    @pl.when(c == 1)
    def _():
        part_copy().wait_recv()
        part[1] = part[0] + p1[0]
        for k, device in same_lo.items():
            remote(part.at[1], p3.at[shards + k - 1], small_send.at[1], small_recv.at[1], device).start()
        for k in range(shards):
            remote(part.at[1], p3.at[k], small_send.at[1], small_recv.at[1], where(k)).start()
        remote(p3, p3, small_send.at[1], small_recv.at[1], where(0)).wait()
        part[2] = part[1] + jnp.sum(p3[...], axis=0)
        for k, device in column.items():
            remote(part.at[2], p2.at[k - 1], small_send.at[2], small_recv.at[2], device).start()
        remote(p2, p2, small_send.at[2], small_recv.at[2], column[1]).wait()
        whole[0] = part[2] + jnp.sum(p2[...], axis=0)
        sum_copy().start()

    mean = whole[0] / count
    clip = jnp.max(jnp.minimum(1.0, CLIP_LEVEL / jnp.sqrt(mean + 1e-06)))

    def nesterov_of(gradient, momentum):
        pulled = clip * gradient.astype(jnp.float32)
        return (pulled + MOMENTUM_DECAY * (MOMENTUM_DECAY * momentum.astype(jnp.float32) + pulled)).astype(jnp.bfloat16)

    def nesterov_copy(i):
        k = early + lax.rem(i + turn, shards - early)
        return k, remote(nest.at[k], got.at[k], send_sem.at[k], recv_sem.at[k], where(k))

    def send_nesterov(i, _):
        k, copy = nesterov_copy(i)
        nest[k] = nesterov_of(pair_v[k, 0], m_v[index(k)])
        copy.start()
        return 0

    lax.fori_loop(0, shards - early, send_nesterov, 0)

    def add_pair(k, total):
        remote(pair_v.at[k], got_pair.at[k], send_sem.at[k], pair_recv.at[k], where(k)).wait_recv()
        block = nesterov_of(got_pair[k, 0], got_pair[k, 1])
        got[k] = block
        wide = block.astype(jnp.float32)
        return total + wide * wide

    def add_nesterov(k, total):
        remote(nest.at[k], got.at[k], send_sem.at[k], recv_sem.at[k], where(k)).wait_recv()
        wide = got[k].astype(jnp.float32)
        return total + wide * wide

    total = lax.fori_loop(early, shards, add_nesterov, lax.fori_loop(0, early, add_pair, nothing))

    norm = jnp.sqrt(jnp.full((1, LANES), jnp.sum(total), jnp.float32))
    scale = jnp.max(1.0 / (norm + 1e-07))
    square_row[...] = norm
    for k in range(shards):
        remote(square_row, squares.at[k], small_send.at[3], small_recv.at[3], where(k)).start()
    for k in range(0, shards, 2):
        pair = jnp.concatenate([got[k].astype(jnp.float32), got[k + 1].astype(jnp.float32)], axis=0)
        mat[pl.ds(k * rows, 2 * rows), :] = (pair * scale).astype(jnp.bfloat16)

    over = (((1,), (1,)), ((), ()))
    plain = (((1,), (0,)), ((), ()))
    full = shards * rows
    for repeat in range(ITERS):
        iterate = mat[...]
        gram_v[...] = lax.dot_general(iterate, iterate, over, preferred_element_type=jnp.float32).astype(jnp.bfloat16)
        gram = gram_v[...]
        squared_gram = lax.dot_general(gram, gram, plain, preferred_element_type=jnp.float32)
        gram_v[...] = (QUINTIC_B * gram.astype(jnp.float32) + QUINTIC_C * squared_gram).astype(jnp.bfloat16)
        if repeat < ITERS - 1:
            product = lax.dot_general(gram_v[...], iterate, plain, preferred_element_type=jnp.float32)
            mat[...] = (QUINTIC_A * iterate.astype(jnp.float32) + product).astype(jnp.bfloat16)

    chunk = 4 if shards % 4 == 0 else 2
    for i in range(shards // chunk):
        first = lax.rem(i + turn, shards // chunk) * chunk
        span = pl.ds(pl.multiple_of(first * rows, chunk * rows), chunk * rows)
        product = lax.dot_general(gram_v[span, :], mat[...], plain, preferred_element_type=jnp.float32)
        final = (QUINTIC_A * mat[span, :].astype(jnp.float32) + product) * math.sqrt(cols)
        for k in range(chunk):
            back[first + k] = final[k * rows:(k + 1) * rows].astype(jnp.bfloat16)
            remote(back.at[first + k], upd_ref.at[me], back_send, back_recv, where(first + k)).start()

    def keep(k, _):
        j = index(k)
        mom_ref[j] = MOMENTUM_DECAY * m_v[j] + clip * pair_v[k, 0].astype(jnp.float32)
        return 0

    lax.fori_loop(0, shards, keep, 0)

    remote(squares, squares, small_send.at[3], small_recv.at[3], where(0)).wait()
    owner_load.wait()
    taken = jnp.int32(0)
    slots = [jnp.zeros((1, LANES), jnp.float32) for _ in range(CAP)]
    named = [(index(k), squares[k] / math.sqrt(full * cols)) for k in range(shards)]
    for j in range(mats):
        mine = (owner_ref[0, j] == me).astype(jnp.int32)
        rank = taken
        taken = taken + mine
        for s in range(CAP):
            hit = mine * (rank == s).astype(jnp.int32)
            for place, value in named:
                slots[s] = slots[s] + (hit * (place == j).astype(jnp.int32)).astype(jnp.float32) * value
    lane = lax.broadcasted_iota(jnp.int32, (1, LANES), 1)
    slot_ref[0] = jnp.where(lane == 0, slots[0], slots[1])[:, :CAP]

    def pair_left(k, _):
        remote(pair_v.at[k], got_pair.at[k], send_sem.at[k], pair_recv.at[k], where(k)).wait_send()
        return 0

    def nesterov_left(i, _):
        nesterov_copy(i)[1].wait_send()
        return 0

    lax.fori_loop(0, early, pair_left, 0)
    lax.fori_loop(0, shards - early, nesterov_left, 0)

    @pl.when(c == 1)
    def _():
        sum_copy().wait_send()

    remote(upd_ref, upd_ref, back_send, back_recv, where(0)).wait()


def finish(*refs):
    sources, targets, sem = refs[:3], refs[3:6], refs[6]
    copies = [pltpu.make_async_copy(a, b, sem.at[i]) for i, (a, b) in enumerate(zip(sources, targets))]
    for copy in copies:
        copy.start()
    for copy in copies:
        copy.wait()


def body(gradient, momentum, owner):
    sizes = (lax.axis_size("z"), lax.axis_size("yh"), lax.axis_size("x"))
    shards = sizes[1] * sizes[2]
    _, mats, rows, cols = gradient.shape
    count = mats * rows * cols * shards * lax.axis_size(GRP)
    full = rows * shards
    far, vmem = pl.BlockSpec(memory_space=pltpu.HBM), pl.BlockSpec(memory_space=pltpu.VMEM)
    dma = pltpu.SemaphoreType.DMA
    arguments = (gradient[0], momentum[0], owner.reshape(1, mats))
    results = pl.pallas_call(
        functools.partial(kernel, sizes, count),
        name="muon",
        out_shape=(
            pltpu.VMEM((mats, rows, cols), jnp.bfloat16),
            pltpu.VMEM((mats, rows, cols), jnp.float32),
            pltpu.VMEM((1, 1, CAP), jnp.float32),
        ),
        in_specs=[far] * 3,
        out_specs=(vmem,) * 3,
        scratch_shapes=[
            pltpu.SMEM((1, mats), jnp.int32),
            pltpu.VMEM((shards, 2, rows, cols), jnp.bfloat16),
            pltpu.VMEM((mats, rows, cols), jnp.float32),
            pltpu.VMEM((shards, 2, rows, cols), jnp.bfloat16),
            pltpu.VMEM((shards, rows, cols), jnp.bfloat16),
            pltpu.VMEM((shards, rows, cols), jnp.bfloat16),
            pltpu.VMEM((full, cols), jnp.bfloat16),
            pltpu.VMEM((shards, rows, cols), jnp.bfloat16),
            pltpu.VMEM((full, full), jnp.bfloat16),
            pltpu.VMEM((3, 1, LANES), jnp.float32),
            pltpu.VMEM((1, 1, LANES), jnp.float32),
            pltpu.VMEM((sizes[0] - 1, 1, LANES), jnp.float32),
            pltpu.VMEM((2 * shards - 1, 1, LANES), jnp.float32),
            pltpu.VMEM((1, 1, LANES), jnp.float32),
            pltpu.VMEM((shards, 1, LANES), jnp.float32),
            pltpu.VMEM((1, LANES), jnp.float32),
            dma((shards,)),
            dma((2,)),
            dma((shards,)),
            dma((shards,)),
            dma((shards,)),
            dma,
            dma,
            dma((5,)),
            dma((5,)),
        ],
        compiler_params=pltpu.CompilerParams(collective_id=0, has_side_effects=True, vmem_limit_bytes=24 << 20),
    )(*(pltpu.with_memory_space_constraint(a, pltpu.HBM) for a in arguments))
    update, momentum_out, slots = pl.pallas_call(
        finish,
        name="finish",
        out_shape=tuple(jax.ShapeDtypeStruct(a.shape, a.dtype) for a in results),
        in_specs=[vmem] * 3,
        out_specs=(far,) * 3,
        scratch_shapes=[dma((3,))],
        compiler_params=pltpu.CompilerParams(vmem_limit_bytes=8 << 20),
    )(*results)
    return update[None], momentum_out[None], slots


def solution(mesh):
    finer = Mesh(mesh.devices.reshape(12, 2, 2, 4, 4), AXES)
    return jax.shard_map(
        body,
        mesh=finer,
        in_specs=(P(GRP, None, SHARD, None), P(GRP, None, SHARD, None), P(GRP, None, None)),
        out_specs=(P(GRP, None, SHARD, None), P(GRP, None, SHARD, None), P(GRP, SHARD, None)),
        check_vma=False,
    )
```

```python
import functools
import math

import jax
import jax.numpy as jnp
from jax import lax
from jax.experimental import pallas as pl
from jax.experimental.pallas import tpu as pltpu
from jax.sharding import Mesh
from jax.sharding import PartitionSpec as P

ITERS = 3
CAP = 2
QUINTIC_A = 3.4445
QUINTIC_B = -4.775
QUINTIC_C = 2.0315
MOMENTUM_DECAY = 0.95
CLIP_LEVEL = 0.5

AXES = ("z", "yl", "c", "yh", "x")
SHARD = ("yh", "x")
GRP = ("z", "yl", "c")
LANES = 128
ALL_UP_TO = 4
LATE_TAIL = 4
HOLD = 2


def up_to(z, last):
    return lax.div(12 + last - z, 12)


def early_blocks(z, shards):
    return shards - shards // LATE_TAIL * (1 - up_to(z, ALL_UP_TO))


def kernel(sizes, count, g_hbm, m_hbm, owner_hbm, upd_ref, mom_ref, slot_ref,
           owner_ref, pair_v, m_v, got_pair, nest, got, mat, back, gram_v, part, p1, p2, p3, whole, squares, square_row,
           g_sem, load_sem, send_sem, pair_recv, recv_sem, back_send, back_recv, small_send, small_recv, go_sem, late_sem, column_sem, ready_sem):
    z_size, yh_size, x_size = sizes
    mats, rows, cols = m_v.shape
    shards = yh_size * x_size
    z, yl, c = lax.axis_index("z"), lax.axis_index("yl"), lax.axis_index("c")
    yh, x = lax.axis_index("yh"), lax.axis_index("x")
    me = yh * x_size + x
    tail = shards - early_blocks(z, shards)
    early = (1 - c) * (shards - tail)
    turn = me + 2 * yl
    late = (z + yl + c + me == 0).astype(jnp.int32)
    beside_late = (z + (1 - yl) == 0).astype(jnp.int32)
    meets_late = beside_late * (1 - c)
    its_place = x * yh_size + lax.rem(yh + yh_size - 1, yh_size)
    its_time = shards // 2 + lax.rem(me, shards // 2)
    pair_turn = meets_late * (its_place + shards - its_time) + (1 - meets_late) * turn

    def peer(k):
        h, dx = lax.rem(k + 1, yh_size), lax.div(k, yh_size)
        there_h = lax.rem(yh + h * (1 - yl) + (yh_size - h) * yl, yh_size)
        there_x = lax.rem(x + dx * (1 - yl) + (x_size - dx) * yl, x_size)
        return there_h, there_x

    def where(k):
        there_h, there_x = peer(jnp.int32(k))
        return {"z": z, "yl": 1 - yl, "c": c, "yh": there_h, "x": there_x}

    def index(k):
        there_h, there_x = peer(jnp.int32(k))
        return there_h * x_size + there_x

    def remote(source, target, sender, receiver, device):
        return pltpu.make_async_remote_copy(source, target, sender, receiver, device_id=device)

    here = {"z": z, "yl": yl, "c": c, "yh": yh, "x": x}
    other_core = {**here, "c": 1 - c}
    far_first = sorted(range(1, z_size), key=lambda k: -min(k, z_size - k))
    column = {k: {**here, "z": lax.rem(z + k, z_size)} for k in far_first}
    same_lo = {k: {**here, "yh": lax.rem(yh + k // x_size, yh_size), "x": lax.rem(x + k % x_size, x_size)} for k in range(1, shards)}

    barrier = pltpu.get_barrier_semaphore()

    @pl.when(c == 1)
    def _():
        for device in same_lo.values():
            pl.semaphore_signal(barrier, inc=1, device_id=device)
        for k, device in column.items():

            @pl.when(z + k < z_size)
            def _():
                pl.semaphore_signal(barrier, inc=1, device_id=device)

    @pl.when(late == 0)
    def _():
        for k in range(shards):
            pl.semaphore_signal(barrier, inc=1, device_id={**where(k), "c": 1})

    pl.semaphore_signal(barrier, inc=1, device_id=other_core)

    def g_load(k):
        return pltpu.make_async_copy(g_hbm.at[index(k)], pair_v.at[k, 0], g_sem.at[k])

    for k in range(shards):
        g_load(k).start()
    m_load = pltpu.make_async_copy(m_hbm, m_v, load_sem.at[0])
    m_load.start()
    owner_load = pltpu.make_async_copy(owner_hbm, owner_ref, load_sem.at[1])
    owner_load.start()

    def add_gradient(k, total):
        g_load(k).wait()
        wide = pair_v[k, 0].astype(jnp.float32)
        return total + wide * wide

    nothing = jnp.zeros((rows, cols), jnp.float32)
    part[0] = jnp.full((1, LANES), jnp.sum(lax.fori_loop(0, shards, add_gradient, nothing)), jnp.float32)

    pl.semaphore_wait(barrier, 1 + c * (2 * shards - beside_late + z + len(same_lo)))

    def part_copy():
        return remote(part.at[0], p1.at[0], small_send.at[0], small_recv.at[0], other_core)

    def sum_copy():
        return remote(whole.at[0], whole.at[0], small_send.at[4], small_recv.at[4], other_core)

    @pl.when(c == 0)
    def _():
        part_copy().start()
        pl.semaphore_wait(ready_sem, 1)

        @pl.when(late == 1)
        def _():
            for k in range(shards):
                pl.semaphore_signal(late_sem, inc=1, device_id=where(k))

    @pl.when(c == 1)
    def _():
        pl.semaphore_signal(ready_sem, inc=1, device_id=other_core)
        part_copy().wait_recv()
        part[1] = part[0] + p1[0]
        for k, device in same_lo.items():
            remote(part.at[1], p3.at[shards + k - 1], small_send.at[1], small_recv.at[1], device).start()
        for k in range(shards):
            remote(part.at[1], p3.at[k], small_send.at[1], small_recv.at[1], where(k)).start()
        for k, device in column.items():

            @pl.when(z + k >= z_size)
            def _():
                pl.semaphore_signal(column_sem, inc=1, device_id=device)

    m_load.wait()

    def send_pair(i, _):
        k = lax.rem(i + pair_turn, early)
        pair_v[k, 1] = m_v[index(k)].astype(jnp.bfloat16)
        remote(pair_v.at[k], got_pair.at[k], send_sem.at[k], pair_recv.at[k], where(k)).start()
        return 0

    lax.fori_loop(0, lax.div(early, 2), send_pair, 0)

    @pl.when(meets_late == 1)
    def _():
        pl.semaphore_wait(late_sem, 1)

    lax.fori_loop(lax.div(early, 2), early, send_pair, 0)

    @pl.when(c == 0)
    def _():
        part_copy().wait_send()
        sum_copy().wait_recv()

    @pl.when(c == 1)
    def _():
        remote(p3, p3, small_send.at[1], small_recv.at[1], where(0)).wait()
        part[2] = part[1] + jnp.sum(p3[...], axis=0)

        @pl.when(z < z_size - 1)
        def _():
            pl.semaphore_wait(column_sem, z_size - 1 - z)

        for k, device in column.items():
            remote(part.at[2], p2.at[k - 1], small_send.at[2], small_recv.at[2], device).start()
        remote(p2, p2, small_send.at[2], small_recv.at[2], column[1]).wait()
        whole[0] = part[2] + jnp.sum(p2[...], axis=0)
        sum_copy().start()

    mean = whole[0] / count
    clip = jnp.max(jnp.minimum(1.0, CLIP_LEVEL / jnp.sqrt(mean + 1e-06)))

    def nesterov_of(gradient, momentum):
        pulled = clip * gradient.astype(jnp.float32)
        return (pulled + MOMENTUM_DECAY * (MOMENTUM_DECAY * momentum.astype(jnp.float32) + pulled)).astype(jnp.bfloat16)

    def nesterov_copy(i):
        k = early + lax.rem(i + turn, shards - early)
        return k, remote(nest.at[k], got.at[k], send_sem.at[k], recv_sem.at[k], where(k))

    def make_nesterov(i, _):
        k, copy = nesterov_copy(i)
        nest[k] = nesterov_of(pair_v[k, 0], m_v[index(k)])

        @pl.when(c * tail == 0)
        def _():
            copy.start()

        return 0

    def send_nesterov(i, _):
        nesterov_copy(i)[1].start()
        return 0

    def nesterov_left(i, _):
        nesterov_copy(i)[1].wait_send()
        return 0

    lax.fori_loop(0, shards - early, make_nesterov, 0)

    @pl.when((1 - c) * tail > 0)
    def _():
        lax.fori_loop(0, tail - HOLD, nesterov_left, 0)
        pl.semaphore_signal(go_sem, inc=1, device_id=other_core)

    @pl.when(c * tail > 0)
    def _():
        pl.semaphore_wait(go_sem, 1)
        lax.fori_loop(0, shards - early, send_nesterov, 0)

    def add_pair(k, total):
        remote(pair_v.at[k], got_pair.at[k], send_sem.at[k], pair_recv.at[k], where(k)).wait_recv()
        block = nesterov_of(got_pair[k, 0], got_pair[k, 1])
        got[k] = block
        wide = block.astype(jnp.float32)
        return total + wide * wide

    def add_nesterov(k, total):
        remote(nest.at[k], got.at[k], send_sem.at[k], recv_sem.at[k], where(k)).wait_recv()
        wide = got[k].astype(jnp.float32)
        return total + wide * wide

    total = lax.fori_loop(early, shards, add_nesterov, lax.fori_loop(0, early, add_pair, nothing))

    norm = jnp.sqrt(jnp.full((1, LANES), jnp.sum(total), jnp.float32))
    scale = jnp.max(1.0 / (norm + 1e-07))
    square_row[...] = norm
    for k in range(shards):
        remote(square_row, squares.at[k], small_send.at[3], small_recv.at[3], where(k)).start()
    for k in range(0, shards, 2):
        pair = jnp.concatenate([got[k].astype(jnp.float32), got[k + 1].astype(jnp.float32)], axis=0)
        mat[pl.ds(k * rows, 2 * rows), :] = (pair * scale).astype(jnp.bfloat16)

    over = (((1,), (1,)), ((), ()))
    plain = (((1,), (0,)), ((), ()))
    full = shards * rows
    for repeat in range(ITERS):
        iterate = mat[...]
        gram_v[...] = lax.dot_general(iterate, iterate, over, preferred_element_type=jnp.float32).astype(jnp.bfloat16)
        gram = gram_v[...]
        squared_gram = lax.dot_general(gram, gram, plain, preferred_element_type=jnp.float32)
        gram_v[...] = (QUINTIC_B * gram.astype(jnp.float32) + QUINTIC_C * squared_gram).astype(jnp.bfloat16)
        if repeat < ITERS - 1:
            product = lax.dot_general(gram_v[...], iterate, plain, preferred_element_type=jnp.float32)
            mat[...] = (QUINTIC_A * iterate.astype(jnp.float32) + product).astype(jnp.bfloat16)

    chunk = 4 if shards % 4 == 0 else 2
    for i in range(shards // chunk):
        first = lax.rem(i + turn, shards // chunk) * chunk
        span = pl.ds(pl.multiple_of(first * rows, chunk * rows), chunk * rows)
        product = lax.dot_general(gram_v[span, :], mat[...], plain, preferred_element_type=jnp.float32)
        final = (QUINTIC_A * mat[span, :].astype(jnp.float32) + product) * math.sqrt(cols)
        for k in range(chunk):
            back[first + k] = final[k * rows:(k + 1) * rows].astype(jnp.bfloat16)
            remote(back.at[first + k], upd_ref.at[me], back_send, back_recv, where(first + k)).start()

    def keep(k, _):
        j = index(k)
        mom_ref[j] = MOMENTUM_DECAY * m_v[j] + clip * pair_v[k, 0].astype(jnp.float32)
        return 0

    lax.fori_loop(0, shards, keep, 0)

    remote(squares, squares, small_send.at[3], small_recv.at[3], where(0)).wait()
    owner_load.wait()
    taken = jnp.int32(0)
    slots = [jnp.zeros((1, LANES), jnp.float32) for _ in range(CAP)]
    named = [(index(k), squares[k] / math.sqrt(full * cols)) for k in range(shards)]
    for j in range(mats):
        mine = (owner_ref[0, j] == me).astype(jnp.int32)
        rank = taken
        taken = taken + mine
        for s in range(CAP):
            hit = mine * (rank == s).astype(jnp.int32)
            for place, value in named:
                slots[s] = slots[s] + (hit * (place == j).astype(jnp.int32)).astype(jnp.float32) * value
    lane = lax.broadcasted_iota(jnp.int32, (1, LANES), 1)
    slot_ref[0] = jnp.where(lane == 0, slots[0], slots[1])[:, :CAP]

    def pair_left(k, _):
        remote(pair_v.at[k], got_pair.at[k], send_sem.at[k], pair_recv.at[k], where(k)).wait_send()
        return 0

    lax.fori_loop(0, early, pair_left, 0)

    @pl.when((1 - c) * tail > 0)
    def _():
        lax.fori_loop(tail - HOLD, tail, nesterov_left, 0)

    @pl.when(c == 1)
    def _():
        lax.fori_loop(0, shards - early, nesterov_left, 0)
        sum_copy().wait_send()

    remote(upd_ref, upd_ref, back_send, back_recv, where(0)).wait()


def finish(*refs):
    sources, targets, sem = refs[:3], refs[3:6], refs[6]
    copies = [pltpu.make_async_copy(a, b, sem.at[i]) for i, (a, b) in enumerate(zip(sources, targets))]
    for copy in copies:
        copy.start()
    for copy in copies:
        copy.wait()


def body(gradient, momentum, owner):
    sizes = (lax.axis_size("z"), lax.axis_size("yh"), lax.axis_size("x"))
    shards = sizes[1] * sizes[2]
    _, mats, rows, cols = gradient.shape
    count = mats * rows * cols * shards * lax.axis_size(GRP)
    full = rows * shards
    far, vmem = pl.BlockSpec(memory_space=pltpu.HBM), pl.BlockSpec(memory_space=pltpu.VMEM)
    dma = pltpu.SemaphoreType.DMA
    arguments = (gradient[0], momentum[0], owner.reshape(1, mats))
    results = pl.pallas_call(
        functools.partial(kernel, sizes, count),
        name="muon",
        out_shape=(
            pltpu.VMEM((mats, rows, cols), jnp.bfloat16),
            pltpu.VMEM((mats, rows, cols), jnp.float32),
            pltpu.VMEM((1, 1, CAP), jnp.float32),
        ),
        in_specs=[far] * 3,
        out_specs=(vmem,) * 3,
        scratch_shapes=[
            pltpu.SMEM((1, mats), jnp.int32),
            pltpu.VMEM((shards, 2, rows, cols), jnp.bfloat16),
            pltpu.VMEM((mats, rows, cols), jnp.float32),
            pltpu.VMEM((shards, 2, rows, cols), jnp.bfloat16),
            pltpu.VMEM((shards, rows, cols), jnp.bfloat16),
            pltpu.VMEM((shards, rows, cols), jnp.bfloat16),
            pltpu.VMEM((full, cols), jnp.bfloat16),
            pltpu.VMEM((shards, rows, cols), jnp.bfloat16),
            pltpu.VMEM((full, full), jnp.bfloat16),
            pltpu.VMEM((3, 1, LANES), jnp.float32),
            pltpu.VMEM((1, 1, LANES), jnp.float32),
            pltpu.VMEM((sizes[0] - 1, 1, LANES), jnp.float32),
            pltpu.VMEM((2 * shards - 1, 1, LANES), jnp.float32),
            pltpu.VMEM((1, 1, LANES), jnp.float32),
            pltpu.VMEM((shards, 1, LANES), jnp.float32),
            pltpu.VMEM((1, LANES), jnp.float32),
            dma((shards,)),
            dma((2,)),
            dma((shards,)),
            dma((shards,)),
            dma((shards,)),
            dma,
            dma,
            dma((5,)),
            dma((5,)),
            pltpu.SemaphoreType.REGULAR,
            pltpu.SemaphoreType.REGULAR,
            pltpu.SemaphoreType.REGULAR,
            pltpu.SemaphoreType.REGULAR,
        ],
        compiler_params=pltpu.CompilerParams(collective_id=0, has_side_effects=True, vmem_limit_bytes=24 << 20),
    )(*(pltpu.with_memory_space_constraint(a, pltpu.HBM) for a in arguments))
    update, momentum_out, slots = pl.pallas_call(
        finish,
        name="finish",
        out_shape=tuple(jax.ShapeDtypeStruct(a.shape, a.dtype) for a in results),
        in_specs=[vmem] * 3,
        out_specs=(far,) * 3,
        scratch_shapes=[dma((3,))],
        compiler_params=pltpu.CompilerParams(vmem_limit_bytes=8 << 20),
    )(*results)
    return update[None], momentum_out[None], slots


def solution(mesh):
    finer = Mesh(mesh.devices.reshape(12, 2, 2, 4, 4), AXES)
    return jax.shard_map(
        body,
        mesh=finer,
        in_specs=(P(GRP, None, SHARD, None), P(GRP, None, SHARD, None), P(GRP, None, None)),
        out_specs=(P(GRP, None, SHARD, None), P(GRP, None, SHARD, None), P(GRP, SHARD, None)),
        check_vma=False,
    )
```

```python
import functools
import math

import jax
import jax.numpy as jnp
from jax import lax
from jax.experimental import pallas as pl
from jax.experimental.pallas import tpu as pltpu
from jax.sharding import Mesh
from jax.sharding import PartitionSpec as P

ITERS = 3
CAP = 2
QUINTIC_A = 3.4445
QUINTIC_B = -4.775
QUINTIC_C = 2.0315
MOMENTUM_DECAY = 0.95
CLIP_LEVEL = 0.5

AXES = ("z", "yl", "c", "yh", "x")
SHARD = ("yh", "x")
GRP = ("z", "yl", "c")
LANES = 128
ALL_UP_TO = 4
LATE_TAIL = 4
HOLD = 2


def up_to(z, last):
    return lax.div(12 + last - z, 12)


def early_blocks(z, shards):
    return shards - shards // LATE_TAIL * (1 - up_to(z, ALL_UP_TO))


def kernel(sizes, count, g_hbm, m_hbm, owner_hbm, upd_ref, mom_ref, slot_ref,
           owner_ref, pair_v, m_v, got_pair, nest, got, mat, back, gram_v, part, p1, p2, p3, whole, squares, square_row,
           g_sem, load_sem, send_sem, pair_recv, recv_sem, back_send, back_recv, small_send, small_recv, go_sem, late_sem, column_sem, ready_sem):
    z_size, yh_size, x_size = sizes
    mats, rows, cols = m_v.shape
    shards = yh_size * x_size
    z, yl, c = lax.axis_index("z"), lax.axis_index("yl"), lax.axis_index("c")
    yh, x = lax.axis_index("yh"), lax.axis_index("x")
    me = yh * x_size + x
    tail = shards - early_blocks(z, shards)
    early = (1 - c) * (shards - tail)
    turn = me + 2 * yl
    late = (z + yl + c + me == 0).astype(jnp.int32)
    beside_late = (z + (1 - yl) == 0).astype(jnp.int32)
    meets_late = beside_late * (1 - c)
    its_place = x * yh_size + lax.rem(yh + yh_size - 1, yh_size)
    its_time = shards // 2 + lax.rem(me, shards // 2)
    pair_turn = meets_late * (its_place + shards - its_time) + (1 - meets_late) * turn

    def peer(k):
        h, dx = lax.rem(k + 1, yh_size), lax.div(k, yh_size)
        there_h = lax.rem(yh + h * (1 - yl) + (yh_size - h) * yl, yh_size)
        there_x = lax.rem(x + dx * (1 - yl) + (x_size - dx) * yl, x_size)
        return there_h, there_x

    def where(k):
        there_h, there_x = peer(jnp.int32(k))
        return {"z": z, "yl": 1 - yl, "c": c, "yh": there_h, "x": there_x}

    def index(k):
        there_h, there_x = peer(jnp.int32(k))
        return there_h * x_size + there_x

    def remote(source, target, sender, receiver, device):
        return pltpu.make_async_remote_copy(source, target, sender, receiver, device_id=device)

    here = {"z": z, "yl": yl, "c": c, "yh": yh, "x": x}
    other_core = {**here, "c": 1 - c}
    far_first = sorted(range(1, z_size), key=lambda k: -min(k, z_size - k))
    column = {k: {**here, "z": lax.rem(z + k, z_size)} for k in far_first}
    same_lo = {k: {**here, "yh": lax.rem(yh + k // x_size, yh_size), "x": lax.rem(x + k % x_size, x_size)} for k in range(1, shards)}

    barrier = pltpu.get_barrier_semaphore()

    @pl.when(c == 1)
    def _():
        for device in same_lo.values():
            pl.semaphore_signal(barrier, inc=1, device_id=device)
        for k, device in column.items():

            @pl.when(z + k < z_size)
            def _():
                pl.semaphore_signal(barrier, inc=1, device_id=device)

    @pl.when(late == 0)
    def _():
        for k in range(shards):
            pl.semaphore_signal(barrier, inc=1, device_id={**where(k), "c": 1})

    pl.semaphore_signal(barrier, inc=1, device_id=other_core)

    def g_load(k):
        return pltpu.make_async_copy(g_hbm.at[index(k)], pair_v.at[k, 0], g_sem.at[k])

    for k in range(shards):
        g_load(k).start()
    m_load = pltpu.make_async_copy(m_hbm, m_v, load_sem.at[0])
    m_load.start()
    owner_load = pltpu.make_async_copy(owner_hbm, owner_ref, load_sem.at[1])
    owner_load.start()

    def add_gradient(k, total):
        g_load(k).wait()
        wide = pair_v[k, 0].astype(jnp.float32)
        return total + wide * wide

    nothing = jnp.zeros((rows, cols), jnp.float32)
    part[0] = jnp.full((1, LANES), jnp.sum(lax.fori_loop(0, shards, add_gradient, nothing)), jnp.float32)

    pl.semaphore_wait(barrier, 1 + c * (2 * shards - beside_late + z + len(same_lo)))

    def part_copy():
        return remote(part.at[0], p1.at[0], small_send.at[0], small_recv.at[0], other_core)

    def sum_copy():
        return remote(whole.at[0], whole.at[0], small_send.at[4], small_recv.at[4], other_core)

    @pl.when(c == 0)
    def _():
        part_copy().start()
        pl.semaphore_wait(ready_sem, 1)

        @pl.when(late == 1)
        def _():
            for k in range(shards):
                pl.semaphore_signal(late_sem, inc=1, device_id=where(k))

    @pl.when(c == 1)
    def _():
        pl.semaphore_signal(ready_sem, inc=1, device_id=other_core)
        part_copy().wait_recv()
        part[1] = part[0] + p1[0]
        for k, device in same_lo.items():
            remote(part.at[1], p3.at[shards + k - 1], small_send.at[1], small_recv.at[1], device).start()
        for k in range(shards):
            remote(part.at[1], p3.at[k], small_send.at[1], small_recv.at[1], where(k)).start()
        for k, device in column.items():

            @pl.when(z + k >= z_size)
            def _():
                pl.semaphore_signal(column_sem, inc=1, device_id=device)

    m_load.wait()

    def send_pair(i, _):
        k = lax.rem(i + pair_turn, early)
        pair_v[k, 1] = m_v[index(k)].astype(jnp.bfloat16)
        remote(pair_v.at[k], got_pair.at[k], send_sem.at[k], pair_recv.at[k], where(k)).start()
        return 0

    lax.fori_loop(0, lax.div(early, 2), send_pair, 0)

    @pl.when(meets_late == 1)
    def _():
        pl.semaphore_wait(late_sem, 1)

    lax.fori_loop(lax.div(early, 2), early, send_pair, 0)

    @pl.when(c == 0)
    def _():
        part_copy().wait_send()
        sum_copy().wait_recv()

    @pl.when(c == 1)
    def _():
        remote(p3, p3, small_send.at[1], small_recv.at[1], where(0)).wait()
        part[2] = part[1] + jnp.sum(p3[...], axis=0)

        @pl.when(z < z_size - 1)
        def _():
            pl.semaphore_wait(column_sem, z_size - 1 - z)

        for k, device in column.items():
            remote(part.at[2], p2.at[k - 1], small_send.at[2], small_recv.at[2], device).start()
        remote(p2, p2, small_send.at[2], small_recv.at[2], column[1]).wait()
        whole[0] = part[2] + jnp.sum(p2[...], axis=0)
        sum_copy().start()

    mean = whole[0] / count
    clip = jnp.max(jnp.minimum(1.0, CLIP_LEVEL / jnp.sqrt(mean + 1e-06)))

    def nesterov_of(gradient, momentum):
        pulled = clip * gradient.astype(jnp.float32)
        return (pulled + MOMENTUM_DECAY * (MOMENTUM_DECAY * momentum.astype(jnp.float32) + pulled)).astype(jnp.bfloat16)

    def nesterov_copy(i):
        k = early + lax.rem(i + turn, shards - early)
        return k, remote(nest.at[k], got.at[k], send_sem.at[k], recv_sem.at[k], where(k))

    def make_nesterov(i, _):
        k, copy = nesterov_copy(i)
        nest[k] = nesterov_of(pair_v[k, 0], m_v[index(k)])

        @pl.when(c * tail == 0)
        def _():
            copy.start()

        return 0

    def send_nesterov(i, _):
        nesterov_copy(i)[1].start()
        return 0

    def nesterov_left(i, _):
        nesterov_copy(i)[1].wait_send()
        return 0

    lax.fori_loop(0, shards - early, make_nesterov, 0)

    @pl.when((1 - c) * tail > 0)
    def _():
        lax.fori_loop(0, tail - HOLD, nesterov_left, 0)
        pl.semaphore_signal(go_sem, inc=1, device_id=other_core)

    @pl.when(c * tail > 0)
    def _():
        pl.semaphore_wait(go_sem, 1)
        lax.fori_loop(0, shards - early, send_nesterov, 0)

    def add_pair(k, total):
        remote(pair_v.at[k], got_pair.at[k], send_sem.at[k], pair_recv.at[k], where(k)).wait_recv()
        block = nesterov_of(got_pair[k, 0], got_pair[k, 1])
        got[k] = block
        wide = block.astype(jnp.float32)
        return total + wide * wide

    def add_nesterov(k, total):
        remote(nest.at[k], got.at[k], send_sem.at[k], recv_sem.at[k], where(k)).wait_recv()
        wide = got[k].astype(jnp.float32)
        return total + wide * wide

    total = lax.fori_loop(early, shards, add_nesterov, lax.fori_loop(0, early, add_pair, nothing))

    norm = jnp.sqrt(jnp.full((1, LANES), jnp.sum(total), jnp.float32))
    scale = jnp.max(1.0 / (norm + 1e-07))
    square_row[...] = norm
    for k in range(shards):
        remote(square_row, squares.at[k], small_send.at[3], small_recv.at[3], where(k)).start()
    for k in range(0, shards, 2):
        pair = jnp.concatenate([got[k].astype(jnp.float32), got[k + 1].astype(jnp.float32)], axis=0)
        mat[pl.ds(k * rows, 2 * rows), :] = (pair * scale).astype(jnp.bfloat16)

    over = (((1,), (1,)), ((), ()))
    plain = (((1,), (0,)), ((), ()))
    full = shards * rows
    for repeat in range(ITERS):
        iterate = mat[...]
        gram_v[...] = lax.dot_general(iterate, iterate, over, preferred_element_type=jnp.float32).astype(jnp.bfloat16)
        gram = gram_v[...]
        squared_gram = lax.dot_general(gram, gram, plain, preferred_element_type=jnp.float32)
        gram_v[...] = (QUINTIC_B * gram.astype(jnp.float32) + QUINTIC_C * squared_gram).astype(jnp.bfloat16)
        if repeat < ITERS - 1:
            product = lax.dot_general(gram_v[...], iterate, plain, preferred_element_type=jnp.float32)
            mat[...] = (QUINTIC_A * iterate.astype(jnp.float32) + product).astype(jnp.bfloat16)

    chunk = yh_size
    facing = 1 - 2 * yl
    odd = lax.rem(x, 2)
    columns = (0, 1, 3 - odd, 2 + odd)
    for i in range(shards // chunk):
        first = lax.rem((columns[i] - x) * facing + 2 * x_size, x_size) * chunk
        span = pl.ds(pl.multiple_of(first * rows, chunk * rows), chunk * rows)
        product = lax.dot_general(gram_v[span, :], mat[...], plain, preferred_element_type=jnp.float32)
        final = (QUINTIC_A * mat[span, :].astype(jnp.float32) + product) * math.sqrt(cols)
        for k in range(chunk):
            back[first + k] = final[k * rows:(k + 1) * rows].astype(jnp.bfloat16)
        for there in sorted(range(yh_size), key=lambda h: min(h, yh_size - h)):
            k = first + lax.rem((there - yh) * facing + 3 * yh_size - 1, yh_size)
            remote(back.at[k], upd_ref.at[me], back_send, back_recv, where(k)).start()

    def keep(k, _):
        j = index(k)
        mom_ref[j] = MOMENTUM_DECAY * m_v[j] + clip * pair_v[k, 0].astype(jnp.float32)
        return 0

    lax.fori_loop(0, shards, keep, 0)

    remote(squares, squares, small_send.at[3], small_recv.at[3], where(0)).wait()
    owner_load.wait()
    taken = jnp.int32(0)
    slots = [jnp.zeros((1, LANES), jnp.float32) for _ in range(CAP)]
    named = [(index(k), squares[k] / math.sqrt(full * cols)) for k in range(shards)]
    for j in range(mats):
        mine = (owner_ref[0, j] == me).astype(jnp.int32)
        rank = taken
        taken = taken + mine
        for s in range(CAP):
            hit = mine * (rank == s).astype(jnp.int32)
            for place, value in named:
                slots[s] = slots[s] + (hit * (place == j).astype(jnp.int32)).astype(jnp.float32) * value
    lane = lax.broadcasted_iota(jnp.int32, (1, LANES), 1)
    slot_ref[0] = jnp.where(lane == 0, slots[0], slots[1])[:, :CAP]

    def pair_left(k, _):
        remote(pair_v.at[k], got_pair.at[k], send_sem.at[k], pair_recv.at[k], where(k)).wait_send()
        return 0

    lax.fori_loop(0, early, pair_left, 0)

    @pl.when((1 - c) * tail > 0)
    def _():
        lax.fori_loop(tail - HOLD, tail, nesterov_left, 0)

    @pl.when(c == 1)
    def _():
        lax.fori_loop(0, shards - early, nesterov_left, 0)
        sum_copy().wait_send()

    remote(upd_ref, upd_ref, back_send, back_recv, where(0)).wait()


def finish(*refs):
    sources, targets, sem = refs[:3], refs[3:6], refs[6]
    copies = [pltpu.make_async_copy(a, b, sem.at[i]) for i, (a, b) in enumerate(zip(sources, targets))]
    for copy in copies:
        copy.start()
    for copy in copies:
        copy.wait()


def body(gradient, momentum, owner):
    sizes = (lax.axis_size("z"), lax.axis_size("yh"), lax.axis_size("x"))
    shards = sizes[1] * sizes[2]
    _, mats, rows, cols = gradient.shape
    count = mats * rows * cols * shards * lax.axis_size(GRP)
    full = rows * shards
    far, vmem = pl.BlockSpec(memory_space=pltpu.HBM), pl.BlockSpec(memory_space=pltpu.VMEM)
    dma = pltpu.SemaphoreType.DMA
    arguments = (gradient[0], momentum[0], owner.reshape(1, mats))
    results = pl.pallas_call(
        functools.partial(kernel, sizes, count),
        name="muon",
        out_shape=(
            pltpu.VMEM((mats, rows, cols), jnp.bfloat16),
            pltpu.VMEM((mats, rows, cols), jnp.float32),
            pltpu.VMEM((1, 1, CAP), jnp.float32),
        ),
        in_specs=[far] * 3,
        out_specs=(vmem,) * 3,
        scratch_shapes=[
            pltpu.SMEM((1, mats), jnp.int32),
            pltpu.VMEM((shards, 2, rows, cols), jnp.bfloat16),
            pltpu.VMEM((mats, rows, cols), jnp.float32),
            pltpu.VMEM((shards, 2, rows, cols), jnp.bfloat16),
            pltpu.VMEM((shards, rows, cols), jnp.bfloat16),
            pltpu.VMEM((shards, rows, cols), jnp.bfloat16),
            pltpu.VMEM((full, cols), jnp.bfloat16),
            pltpu.VMEM((shards, rows, cols), jnp.bfloat16),
            pltpu.VMEM((full, full), jnp.bfloat16),
            pltpu.VMEM((3, 1, LANES), jnp.float32),
            pltpu.VMEM((1, 1, LANES), jnp.float32),
            pltpu.VMEM((sizes[0] - 1, 1, LANES), jnp.float32),
            pltpu.VMEM((2 * shards - 1, 1, LANES), jnp.float32),
            pltpu.VMEM((1, 1, LANES), jnp.float32),
            pltpu.VMEM((shards, 1, LANES), jnp.float32),
            pltpu.VMEM((1, LANES), jnp.float32),
            dma((shards,)),
            dma((2,)),
            dma((shards,)),
            dma((shards,)),
            dma((shards,)),
            dma,
            dma,
            dma((5,)),
            dma((5,)),
            pltpu.SemaphoreType.REGULAR,
            pltpu.SemaphoreType.REGULAR,
            pltpu.SemaphoreType.REGULAR,
            pltpu.SemaphoreType.REGULAR,
        ],
        compiler_params=pltpu.CompilerParams(collective_id=0, has_side_effects=True, vmem_limit_bytes=24 << 20),
    )(*(pltpu.with_memory_space_constraint(a, pltpu.HBM) for a in arguments))
    update, momentum_out, slots = pl.pallas_call(
        finish,
        name="finish",
        out_shape=tuple(jax.ShapeDtypeStruct(a.shape, a.dtype) for a in results),
        in_specs=[vmem] * 3,
        out_specs=(far,) * 3,
        scratch_shapes=[dma((3,))],
        compiler_params=pltpu.CompilerParams(vmem_limit_bytes=8 << 20),
    )(*results)
    return update[None], momentum_out[None], slots


def solution(mesh):
    finer = Mesh(mesh.devices.reshape(12, 2, 2, 4, 4), AXES)
    return jax.shard_map(
        body,
        mesh=finer,
        in_specs=(P(GRP, None, SHARD, None), P(GRP, None, SHARD, None), P(GRP, None, None)),
        out_specs=(P(GRP, None, SHARD, None), P(GRP, None, SHARD, None), P(GRP, SHARD, None)),
        check_vma=False,
    )
```

```python
import functools
import math

import jax
import jax.numpy as jnp
from jax import lax
from jax.experimental import pallas as pl
from jax.experimental.pallas import tpu as pltpu
from jax.sharding import Mesh
from jax.sharding import PartitionSpec as P

ITERS = 3
CAP = 2
QUINTIC_A = 3.4445
QUINTIC_B = -4.775
QUINTIC_C = 2.0315
MOMENTUM_DECAY = 0.95
CLIP_LEVEL = 0.5

AXES = ("z", "yl", "c", "yh", "x")
SHARD = ("yh", "x")
GRP = ("z", "yl", "c")
LANES = 128
ALL_UP_TO = 4
LATE_TAIL = 4
HOLD = 2


def up_to(z, last):
    return lax.div(12 + last - z, 12)


def early_blocks(z, shards):
    return shards - shards // LATE_TAIL * (1 - up_to(z, ALL_UP_TO))


def kernel(sizes, count, g_hbm, m_hbm, owner_hbm, upd_ref, mom_ref, slot_ref,
           owner_ref, pair_v, m_v, got_pair, nest, got, mat, back, gram_v, part, p1, p2, p3, whole, squares, square_row,
           g_sem, load_sem, send_sem, pair_recv, recv_sem, back_send, back_recv, small_send, small_recv, go_sem, late_sem, column_sem, ready_sem):
    z_size, yh_size, x_size = sizes
    mats, rows, cols = m_v.shape
    shards = yh_size * x_size
    z, yl, c = lax.axis_index("z"), lax.axis_index("yl"), lax.axis_index("c")
    yh, x = lax.axis_index("yh"), lax.axis_index("x")
    me = yh * x_size + x
    tail = shards - early_blocks(z, shards)
    early = (1 - c) * (shards - tail)
    turn = me + 2 * yl
    late = (z + yl + c + me == 0).astype(jnp.int32)
    beside_late = (z + (1 - yl) == 0).astype(jnp.int32)
    meets_late = beside_late * (1 - c)
    its_place = x * yh_size + lax.rem(yh + yh_size - 1, yh_size)
    its_time = shards // 2 + lax.rem(me, shards // 2)
    pair_turn = meets_late * (its_place + shards - its_time) + (1 - meets_late) * turn

    def peer(k):
        h, dx = lax.rem(k + 1, yh_size), lax.div(k, yh_size)
        there_h = lax.rem(yh + h * (1 - yl) + (yh_size - h) * yl, yh_size)
        there_x = lax.rem(x + dx * (1 - yl) + (x_size - dx) * yl, x_size)
        return there_h, there_x

    def where(k):
        there_h, there_x = peer(jnp.int32(k))
        return {"z": z, "yl": 1 - yl, "c": c, "yh": there_h, "x": there_x}

    def index(k):
        there_h, there_x = peer(jnp.int32(k))
        return there_h * x_size + there_x

    def remote(source, target, sender, receiver, device):
        return pltpu.make_async_remote_copy(source, target, sender, receiver, device_id=device)

    here = {"z": z, "yl": yl, "c": c, "yh": yh, "x": x}
    other_core = {**here, "c": 1 - c}
    far_first = sorted(range(1, z_size), key=lambda k: -min(k, z_size - k))
    column = {k: {**here, "z": lax.rem(z + k, z_size)} for k in far_first}
    same_lo = {k: {**here, "yh": lax.rem(yh + k // x_size, yh_size), "x": lax.rem(x + k % x_size, x_size)} for k in range(1, shards)}

    barrier = pltpu.get_barrier_semaphore()

    @pl.when(c == 1)
    def _():
        for device in same_lo.values():
            pl.semaphore_signal(barrier, inc=1, device_id=device)
        for k, device in column.items():

            @pl.when(z + k < z_size)
            def _():
                pl.semaphore_signal(barrier, inc=1, device_id=device)

    @pl.when(late == 0)
    def _():
        for k in range(shards):
            pl.semaphore_signal(barrier, inc=1, device_id={**where(k), "c": 1})

    pl.semaphore_signal(barrier, inc=1, device_id=other_core)

    def g_load(k):
        return pltpu.make_async_copy(g_hbm.at[index(k)], pair_v.at[k, 0], g_sem.at[k])

    for k in range(shards):
        g_load(k).start()
    m_load = pltpu.make_async_copy(m_hbm, m_v, load_sem.at[0])
    m_load.start()
    owner_load = pltpu.make_async_copy(owner_hbm, owner_ref, load_sem.at[1])
    owner_load.start()

    def add_gradient(k, total):
        g_load(k).wait()
        wide = pair_v[k, 0].astype(jnp.float32)
        return total + wide * wide

    nothing = jnp.zeros((rows, cols), jnp.float32)
    part[0] = jnp.full((1, LANES), jnp.sum(lax.fori_loop(0, shards, add_gradient, nothing)), jnp.float32)

    pl.semaphore_wait(barrier, 1 + c * (2 * shards - beside_late + z + len(same_lo)))

    def part_copy():
        return remote(part.at[0], p1.at[0], small_send.at[0], small_recv.at[0], other_core)

    def sum_copy():
        return remote(whole.at[0], whole.at[0], small_send.at[4], small_recv.at[4], other_core)

    @pl.when(c == 0)
    def _():
        part_copy().start()
        pl.semaphore_wait(ready_sem, 1)

        @pl.when(late == 1)
        def _():
            for k in range(shards):
                pl.semaphore_signal(late_sem, inc=1, device_id=where(k))

    @pl.when(c == 1)
    def _():
        pl.semaphore_signal(ready_sem, inc=1, device_id=other_core)
        part_copy().wait_recv()
        part[1] = part[0] + p1[0]
        for k, device in same_lo.items():
            remote(part.at[1], p3.at[shards + k - 1], small_send.at[1], small_recv.at[1], device).start()
        for k in range(shards):
            remote(part.at[1], p3.at[k], small_send.at[1], small_recv.at[1], where(k)).start()
        for k, device in column.items():

            @pl.when(z + k >= z_size)
            def _():
                pl.semaphore_signal(column_sem, inc=1, device_id=device)

    m_load.wait()

    def send_pair(i, _):
        k = lax.rem(i + pair_turn, early)
        pair_v[k, 1] = m_v[index(k)].astype(jnp.bfloat16)
        remote(pair_v.at[k], got_pair.at[k], send_sem.at[k], pair_recv.at[k], where(k)).start()
        return 0

    lax.fori_loop(0, lax.div(early, 2), send_pair, 0)

    @pl.when(meets_late == 1)
    def _():
        pl.semaphore_wait(late_sem, 1)

    lax.fori_loop(lax.div(early, 2), early, send_pair, 0)

    @pl.when(c == 0)
    def _():
        part_copy().wait_send()
        sum_copy().wait_recv()

    @pl.when(c == 1)
    def _():
        remote(p3, p3, small_send.at[1], small_recv.at[1], where(0)).wait()
        part[2] = part[1] + jnp.sum(p3[...], axis=0)

        @pl.when(z < z_size - 1)
        def _():
            pl.semaphore_wait(column_sem, z_size - 1 - z)

        for k, device in column.items():
            remote(part.at[2], p2.at[k - 1], small_send.at[2], small_recv.at[2], device).start()
        remote(p2, p2, small_send.at[2], small_recv.at[2], column[1]).wait()
        whole[0] = part[2] + jnp.sum(p2[...], axis=0)
        sum_copy().start()

    mean = whole[0] / count
    clip = jnp.max(jnp.minimum(1.0, CLIP_LEVEL / jnp.sqrt(mean + 1e-06)))

    def nesterov_of(gradient, momentum):
        pulled = clip * gradient.astype(jnp.float32)
        return (pulled + MOMENTUM_DECAY * (MOMENTUM_DECAY * momentum.astype(jnp.float32) + pulled)).astype(jnp.bfloat16)

    def nesterov_copy(i):
        k = early + lax.rem(i + turn, shards - early)
        return k, remote(nest.at[k], got.at[k], send_sem.at[k], recv_sem.at[k], where(k))

    def make_nesterov(i, _):
        k, copy = nesterov_copy(i)
        nest[k] = nesterov_of(pair_v[k, 0], m_v[index(k)])

        @pl.when(c * tail == 0)
        def _():
            copy.start()

        return 0

    def send_nesterov(i, _):
        nesterov_copy(i)[1].start()
        return 0

    def nesterov_left(i, _):
        nesterov_copy(i)[1].wait_send()
        return 0

    lax.fori_loop(0, shards - early, make_nesterov, 0)

    @pl.when((1 - c) * tail > 0)
    def _():
        lax.fori_loop(0, tail - HOLD, nesterov_left, 0)
        pl.semaphore_signal(go_sem, inc=1, device_id=other_core)

    @pl.when(c * tail > 0)
    def _():
        pl.semaphore_wait(go_sem, 1)
        lax.fori_loop(0, shards - early, send_nesterov, 0)

    def keep_pair(i, blocks):
        wide = jnp.concatenate(blocks, axis=0)
        mat[pl.ds(pl.multiple_of(2 * i * rows, 2 * rows), 2 * rows), :] = wide.astype(jnp.bfloat16)
        return blocks[0] * blocks[0] + blocks[1] * blocks[1]

    def add_pair(i, total):
        blocks = []
        for k in (2 * i, 2 * i + 1):
            remote(pair_v.at[k], got_pair.at[k], send_sem.at[k], pair_recv.at[k], where(k)).wait_recv()
            blocks.append(nesterov_of(got_pair[k, 0], got_pair[k, 1]).astype(jnp.float32))
        return total + keep_pair(i, blocks)

    def add_nesterov(i, total):
        blocks = []
        for k in (2 * i, 2 * i + 1):
            remote(nest.at[k], got.at[k], send_sem.at[k], recv_sem.at[k], where(k)).wait_recv()
            blocks.append(got[k].astype(jnp.float32))
        return total + keep_pair(i, blocks)

    early_pairs = lax.div(early, 2)
    total = lax.fori_loop(early_pairs, shards // 2, add_nesterov, lax.fori_loop(0, early_pairs, add_pair, nothing))

    norm = jnp.sqrt(jnp.full((1, LANES), jnp.sum(total), jnp.float32))
    scale = jnp.max(1.0 / (norm + 1e-07))
    square_row[...] = norm
    for k in range(shards):
        remote(square_row, squares.at[k], small_send.at[3], small_recv.at[3], where(k)).start()

    over = (((1,), (1,)), ((), ()))
    plain = (((1,), (0,)), ((), ()))
    full = shards * rows
    for repeat in range(ITERS):
        iterate = mat[...]
        product = lax.dot_general(iterate, iterate, over, preferred_element_type=jnp.float32)
        if repeat == 0:
            iterate = (iterate.astype(jnp.float32) * scale).astype(jnp.bfloat16)
            product = product * scale * scale
            mat[...] = iterate
        gram = product.astype(jnp.bfloat16)
        squared_gram = lax.dot_general(gram, gram, plain, preferred_element_type=jnp.float32)
        gram_v[...] = (QUINTIC_B * gram.astype(jnp.float32) + QUINTIC_C * squared_gram).astype(jnp.bfloat16)
        if repeat < ITERS - 1:
            product = lax.dot_general(gram_v[...], iterate, plain, preferred_element_type=jnp.float32)
            mat[...] = (QUINTIC_A * iterate.astype(jnp.float32) + product).astype(jnp.bfloat16)

    chunk = yh_size
    facing = 1 - 2 * yl
    odd = lax.rem(x, 2)
    columns = (0, 1, 3 - odd, 2 + odd)
    for i in range(shards // chunk):
        first = lax.rem((columns[i] - x) * facing + 2 * x_size, x_size) * chunk
        span = pl.ds(pl.multiple_of(first * rows, chunk * rows), chunk * rows)
        product = lax.dot_general(gram_v[span, :], mat[...], plain, preferred_element_type=jnp.float32)
        final = (QUINTIC_A * mat[span, :].astype(jnp.float32) + product) * math.sqrt(cols)
        for k in range(chunk):
            back[first + k] = final[k * rows:(k + 1) * rows].astype(jnp.bfloat16)
        for there in sorted(range(yh_size), key=lambda h: min(h, yh_size - h)):
            k = first + lax.rem((there - yh) * facing + 3 * yh_size - 1, yh_size)
            remote(back.at[k], upd_ref.at[me], back_send, back_recv, where(k)).start()

    def keep(k, _):
        j = index(k)
        mom_ref[j] = MOMENTUM_DECAY * m_v[j] + clip * pair_v[k, 0].astype(jnp.float32)
        return 0

    lax.fori_loop(0, shards, keep, 0)

    remote(squares, squares, small_send.at[3], small_recv.at[3], where(0)).wait()
    owner_load.wait()
    taken = jnp.int32(0)
    slots = [jnp.zeros((1, LANES), jnp.float32) for _ in range(CAP)]
    named = [(index(k), squares[k] / math.sqrt(full * cols)) for k in range(shards)]
    for j in range(mats):
        mine = (owner_ref[0, j] == me).astype(jnp.int32)
        rank = taken
        taken = taken + mine
        for s in range(CAP):
            hit = mine * (rank == s).astype(jnp.int32)
            for place, value in named:
                slots[s] = slots[s] + (hit * (place == j).astype(jnp.int32)).astype(jnp.float32) * value
    lane = lax.broadcasted_iota(jnp.int32, (1, LANES), 1)
    slot_ref[0] = jnp.where(lane == 0, slots[0], slots[1])[:, :CAP]

    def pair_left(k, _):
        remote(pair_v.at[k], got_pair.at[k], send_sem.at[k], pair_recv.at[k], where(k)).wait_send()
        return 0

    lax.fori_loop(0, early, pair_left, 0)

    @pl.when((1 - c) * tail > 0)
    def _():
        lax.fori_loop(tail - HOLD, tail, nesterov_left, 0)

    @pl.when(c == 1)
    def _():
        lax.fori_loop(0, shards - early, nesterov_left, 0)
        sum_copy().wait_send()

    remote(upd_ref, upd_ref, back_send, back_recv, where(0)).wait()


def finish(*refs):
    sources, targets, sem = refs[:3], refs[3:6], refs[6]
    copies = [pltpu.make_async_copy(a, b, sem.at[i]) for i, (a, b) in enumerate(zip(sources, targets))]
    for copy in copies:
        copy.start()
    for copy in copies:
        copy.wait()


def body(gradient, momentum, owner):
    sizes = (lax.axis_size("z"), lax.axis_size("yh"), lax.axis_size("x"))
    shards = sizes[1] * sizes[2]
    _, mats, rows, cols = gradient.shape
    count = mats * rows * cols * shards * lax.axis_size(GRP)
    full = rows * shards
    far, vmem = pl.BlockSpec(memory_space=pltpu.HBM), pl.BlockSpec(memory_space=pltpu.VMEM)
    dma = pltpu.SemaphoreType.DMA
    arguments = (gradient[0], momentum[0], owner.reshape(1, mats))
    results = pl.pallas_call(
        functools.partial(kernel, sizes, count),
        name="muon",
        out_shape=(
            pltpu.VMEM((mats, rows, cols), jnp.bfloat16),
            pltpu.VMEM((mats, rows, cols), jnp.float32),
            pltpu.VMEM((1, 1, CAP), jnp.float32),
        ),
        in_specs=[far] * 3,
        out_specs=(vmem,) * 3,
        scratch_shapes=[
            pltpu.SMEM((1, mats), jnp.int32),
            pltpu.VMEM((shards, 2, rows, cols), jnp.bfloat16),
            pltpu.VMEM((mats, rows, cols), jnp.float32),
            pltpu.VMEM((shards, 2, rows, cols), jnp.bfloat16),
            pltpu.VMEM((shards, rows, cols), jnp.bfloat16),
            pltpu.VMEM((shards, rows, cols), jnp.bfloat16),
            pltpu.VMEM((full, cols), jnp.bfloat16),
            pltpu.VMEM((shards, rows, cols), jnp.bfloat16),
            pltpu.VMEM((full, full), jnp.bfloat16),
            pltpu.VMEM((3, 1, LANES), jnp.float32),
            pltpu.VMEM((1, 1, LANES), jnp.float32),
            pltpu.VMEM((sizes[0] - 1, 1, LANES), jnp.float32),
            pltpu.VMEM((2 * shards - 1, 1, LANES), jnp.float32),
            pltpu.VMEM((1, 1, LANES), jnp.float32),
            pltpu.VMEM((shards, 1, LANES), jnp.float32),
            pltpu.VMEM((1, LANES), jnp.float32),
            dma((shards,)),
            dma((2,)),
            dma((shards,)),
            dma((shards,)),
            dma((shards,)),
            dma,
            dma,
            dma((5,)),
            dma((5,)),
            pltpu.SemaphoreType.REGULAR,
            pltpu.SemaphoreType.REGULAR,
            pltpu.SemaphoreType.REGULAR,
            pltpu.SemaphoreType.REGULAR,
        ],
        compiler_params=pltpu.CompilerParams(collective_id=0, has_side_effects=True, vmem_limit_bytes=24 << 20),
    )(*(pltpu.with_memory_space_constraint(a, pltpu.HBM) for a in arguments))
    update, momentum_out, slots = pl.pallas_call(
        finish,
        name="finish",
        out_shape=tuple(jax.ShapeDtypeStruct(a.shape, a.dtype) for a in results),
        in_specs=[vmem] * 3,
        out_specs=(far,) * 3,
        scratch_shapes=[dma((3,))],
        compiler_params=pltpu.CompilerParams(vmem_limit_bytes=8 << 20),
    )(*results)
    return update[None], momentum_out[None], slots


def solution(mesh):
    finer = Mesh(mesh.devices.reshape(12, 2, 2, 4, 4), AXES)
    return jax.shard_map(
        body,
        mesh=finer,
        in_specs=(P(GRP, None, SHARD, None), P(GRP, None, SHARD, None), P(GRP, None, None)),
        out_specs=(P(GRP, None, SHARD, None), P(GRP, None, SHARD, None), P(GRP, SHARD, None)),
        check_vma=False,
    )
```
